32 devices in a mesh: data: 4 (over y, z), expert: 8 (over x, core).
Axes of the slice: x: 4, y: 2, z: 2, core: 2. Of those that a mesh axis runs over, the one named last changes fastest.
The devices are a block of a 4x4x8 slice.
Arguments:
- token_rows: bfloat16 [32768, 2304], P(('data', 'expert')), parts along dimension 0
- expert_ids: int32 [32768, 2], P(('data', 'expert')), parts along dimension 0
- gate_weights: float32 [32768, 2], P(('data', 'expert')), parts along dimension 0
- w_in: bfloat16 [8, 2304, 5760], P('expert')
- w_out: bfloat16 [8, 5760, 2304], P('expert')
Outputs:
- output: bfloat16 [32768, 2304], P(('data', 'expert')), parts along dimension 0
There are 4 independent parts. The reference program is written for one: setup_inputs(seed, part) draws one part's arguments, and reference() takes and returns one part's arrays. A program takes and returns all parts, laid end to end along the dimension named above; an argument that names none is the same for every part.
All inputs are finite; a program needn't handle non-finite values.
Results may differ from the reference program's by a relative error of at most 0.001.
Values are sent between devices in bfloat16 or wider.
A program may use at most 768 MiB of HBM per device.

```python
import math
import jax
import jax.numpy as jnp
from jax import lax

TOKENS_DEV = 1024
GROUP_DEVS = 8
MODEL_DIM = 2304
HIDDEN_DIM = 5760
EXPERTS = 8
TOP_K = 2

TOKENS = TOKENS_DEV * GROUP_DEVS
MEAN_LOAD = TOKENS_DEV * TOP_K // EXPERTS
CAPACITY = TOKENS * TOP_K // EXPERTS
POP_SPREAD = MEAN_LOAD // 2
DEV_SPREAD = MEAN_LOAD // 4


def draw_routing(key):
    key_order, key_pop, key_dev, key_tok, key_col = jax.random.split(key, 5)
    expert_order = jax.random.permutation(key_order, EXPERTS)
    pop_bias = jax.random.randint(key_pop, (EXPERTS,), 0, POP_SPREAD + 1)
    pop_bias = pop_bias.at[0].set(POP_SPREAD).at[1].set(0)
    dev_bias = jax.random.randint(key_dev, (GROUP_DEVS, EXPERTS), 0, DEV_SPREAD + 1)
    dev_bias = dev_bias.at[:, 0].set(DEV_SPREAD).at[:, 1].set(0)
    pair_load = MEAN_LOAD + (pop_bias - jnp.roll(pop_bias, -1))[None, :] + dev_bias - jnp.roll(dev_bias, -1, axis=1)
    run_ends = jnp.cumsum(pair_load, axis=1)
    positions = jnp.arange(TOKENS_DEV * TOP_K, dtype=jnp.int32)

    def find_run(row_ends):
        return jnp.searchsorted(row_ends, positions, side="right")

    run_index = jax.vmap(find_run)(run_ends)
    labels = expert_order[run_index].reshape(GROUP_DEVS, TOP_K, TOKENS_DEV)
    choices = jnp.swapaxes(labels, 1, 2)

    def token_order(sub_key):
        return jax.random.permutation(sub_key, TOKENS_DEV)

    tok_perm = jax.vmap(token_order)(jax.random.split(key_tok, GROUP_DEVS))
    choices = jnp.take_along_axis(choices, tok_perm[:, :, None], axis=1)
    choices = jax.random.permutation(key_col, choices, axis=2, independent=True)
    return choices.reshape(TOKENS, TOP_K).astype(jnp.int32)


def draw_matrices(key, fan_in, fan_out):
    def one_matrix(sub_key):
        return (jax.random.normal(sub_key, (fan_in, fan_out), jnp.float32) / math.sqrt(fan_in)).astype(jnp.bfloat16)
    return lax.map(one_matrix, jax.random.split(key, EXPERTS))


def setup_inputs(seed: int = 0, part: int = 0) -> dict:
    root = jax.random.key(seed)
    part_key = jax.random.fold_in(root, part)
    key_route, key_rows, key_gate = jax.random.split(part_key, 3)
    key_up, key_down = jax.random.split(jax.random.fold_in(root, 1000003), 2)
    token_rows = jax.random.normal(key_rows, (TOKENS, MODEL_DIM), jnp.float32).astype(jnp.bfloat16)
    gate_weights = jax.random.uniform(key_gate, (TOKENS, TOP_K), jnp.float32, 0.5, 1.5) / math.sqrt(TOP_K)
    return {"token_rows": token_rows, "expert_ids": draw_routing(key_route), "gate_weights": gate_weights, "w_in": draw_matrices(key_up, MODEL_DIM, HIDDEN_DIM), "w_out": draw_matrices(key_down, HIDDEN_DIM, MODEL_DIM)}


def expert_ffn(operands):
    rows, up_weight, down_weight = operands
    hidden = jax.nn.gelu(jnp.dot(rows, up_weight, preferred_element_type=jnp.float32)).astype(jnp.bfloat16)
    return jnp.dot(hidden, down_weight, preferred_element_type=jnp.float32).astype(jnp.bfloat16)


def reference(token_rows, expert_ids, gate_weights, w_in, w_out):
    pairs = TOP_K * TOKENS
    flat_ids = expert_ids.T.reshape(pairs)
    sort_order = jnp.argsort(flat_ids, stable=True)
    position = jnp.zeros((pairs,), jnp.int32).at[sort_order].set(jnp.arange(pairs, dtype=jnp.int32))
    counts = jnp.bincount(flat_ids, length=EXPERTS)
    seg_start = jnp.cumsum(counts) - counts
    slot = position - seg_start[flat_ids]
    keep = slot < CAPACITY
    slot_safe = jnp.where(keep, slot, CAPACITY)
    buffer = jnp.zeros((EXPERTS, CAPACITY, MODEL_DIM), token_rows.dtype).at[flat_ids, slot_safe].set(jnp.tile(token_rows, (TOP_K, 1)), mode="drop")
    outputs = lax.map(expert_ffn, (buffer, w_in, w_out))
    weight = jnp.where(keep, gate_weights.T.reshape(pairs), 0.0).reshape(TOP_K, TOKENS)
    slot_read = jnp.minimum(slot, CAPACITY - 1).reshape(TOP_K, TOKENS)

    def add_choice(total, pieces):
        choice_weight, choice_ids, choice_slot = pieces
        return total + choice_weight[:, None] * outputs[choice_ids, choice_slot].astype(jnp.float32), None

    mixed, _ = lax.scan(add_choice, token_rows.astype(jnp.float32), (weight, flat_ids.reshape(TOP_K, TOKENS), slot_read))
    return mixed.astype(jnp.bfloat16)
```

```python
import functools

import jax
import jax.numpy as jnp
from jax import lax
from jax.experimental import pallas as pl
from jax.experimental.pallas import tpu as pltpu
from jax.sharding import PartitionSpec as P

MESH = pl.DeviceIdType.MESH
F32 = jnp.float32
BF16 = jnp.bfloat16


def layer_kernel(cfg, x_ref, ids_ref, gates_ref, win_ref, wout_ref, out_ref, ag_ref, obuf_ref, rbuf_ref,
                 ids_all, slot_tab, comb_tab, ids_send, ids_recv, ag_send, ag_recv, ret_send, ret_recv, barrier_unused=None):
    groups, tokens, dim, hid, cap, slots = cfg
    half = tokens // 2
    chips = groups // 2
    wchunk = 768
    nfull = hid // wchunk
    tail = hid - nfull * wchunk
    ochunks = dim // wchunk

    me = lax.axis_index("expert")
    chip = me // 2
    core = me % 2
    other = 1 - core
    sgn = 1 - 2 * core

    def dev(off, c):
        return ((chip + off + 2 * chips) % chips) * 2 + c

    sib = dev(0, other)
    src_a = dev(-sgn, core)
    src_b = dev(sgn, core)
    far = dev(2, core)

    def tile_dev(t, flip):
        q = t // 2
        p = t % 2
        f1 = q * (2 - q) * (3 - q) // 2
        f2 = q * (q - 1) * (3 - q) // 2
        f3 = q * (q - 1) * (q - 2) // 6
        off = flip * (f1 * (2 * p - 1) + f2 * (1 - 2 * p)) * sgn + 2 * f3
        c = core * (1 - p) + other * p
        return dev(off, c)

    def comb_dev(k):
        q = k // 2
        p = k % 2
        f1 = q * (2 - q) * (3 - q) // 2
        f2 = q * (q - 1) * (3 - q) // 2
        f3 = q * (q - 1) * (q - 2) // 6
        off = (f1 - f2) * sgn + 2 * f3
        c = core * (1 - p) + other * p
        return dev(off, c)

    def remote(src, dst, ssem, rsem, target):
        return pltpu.make_async_remote_copy(src_ref=src, dst_ref=dst, send_sem=ssem, recv_sem=rsem,
                                            device_id={"expert": target}, device_id_type=MESH)

    bar = pltpu.get_barrier_semaphore()
    for k in range(1, groups):
        pl.semaphore_signal(bar, inc=1, device_id={"expert": (me + k) % groups}, device_id_type=MESH)
    pl.semaphore_wait(bar, groups - 1)

    def ids_copy(k):
        return remote(ids_ref, ids_all.at[me], ids_send.at[k - 1], ids_recv.at[me], (me + k) % groups)

    def ag_copy(src, d, h, k, target):
        return remote(src, ag_ref.at[d, pl.ds(h * half, half)], ag_send.at[k], ag_recv.at[2 * d + h], target)

    def own_half(h):
        return x_ref.at[pl.ds(h * half, half)]

    def got_half(d, h):
        return ag_ref.at[d, pl.ds(h * half, half)]

    half_a = (1 - sgn) // 2
    half_b = 1 - half_a
    send_sib = [ag_copy(own_half(h), me, h, h, sib) for h in range(2)]
    send_a = [ag_copy(own_half(h), me, h, 2 + h, src_b) for h in range(2)]
    send_b = [ag_copy(own_half(h), me, h, 4 + h, src_a) for h in range(2)]
    fwd_a = ag_copy(got_half(src_a, half_a), src_a, half_a, 6, src_b)
    fwd_b = ag_copy(got_half(src_b, half_b), src_b, half_b, 7, src_a)
    pass_a = [ag_copy(got_half(src_a, h), src_a, h, 8 + h, sib) for h in range(2)]
    pass_b = [ag_copy(got_half(src_b, h), src_b, h, 10 + h, sib) for h in range(2)]
    pass_f = [ag_copy(got_half(far, h), far, h, 12 + h, sib) for h in range(2)]
    all_sends = send_sib + send_a + send_b + [fwd_a, fwd_b] + pass_a + pass_b + pass_f

    def wait_half(d, h):
        ag_copy(got_half(d, h), d, h, 0, sib).wait_recv()

    def ret_copy(t):
        d = tile_dev(t, 1)
        return remote(obuf_ref.at[d], rbuf_ref.at[me], ret_send.at[t], ret_recv.at[me], d)

    for k in range(1, groups):
        ids_copy(k).start()
    for c in send_sib + send_a:
        c.start()

    def compute(xsrc, xg, hbuf, wbuf, wout, ostage, pbuf, xsem, wsem, osem, stsem, isem):
        own_ids = pltpu.make_async_copy(ids_ref, ids_all.at[me], isem)
        own_ids.start()

        def win_full(i):
            return pltpu.make_async_copy(win_ref.at[:, pl.ds(pl.multiple_of(i * wchunk, 128), wchunk)], wbuf.at[i % 2], wsem.at[i % 2])

        win_tail = pltpu.make_async_copy(win_ref.at[:, pl.ds(nfull * wchunk, tail)], wbuf.at[nfull % 2, :, pl.ds(0, tail)], wsem.at[nfull % 2])

        def wout_part(n):
            return pltpu.make_async_copy(wout_ref.at[:, pl.ds(pl.multiple_of(n * wchunk, 128), wchunk)], wout.at[:, pl.ds(pl.multiple_of(n * wchunk, 128), wchunk)], osem.at[n])

        win_full(0).start()
        for n in range(ochunks):
            wout_part(n).start()

        own_ids.wait()
        for k in range(1, groups):
            ids_copy(k).wait_send()
        for k in range(1, groups):
            d = (me + k) % groups
            remote(ids_ref, ids_all.at[d], ids_send.at[0], ids_recv.at[d], sib).wait_recv()
        ids0 = ids_all[:, 0, :]
        ids1 = ids_all[:, 1, :]
        o0 = ids_ref_v(ids_all, me, 0)
        o1 = ids_ref_v(ids_all, me, 1)
        eidx = lax.broadcasted_iota(jnp.int32, (groups, tokens), 0)

        def ind(m):
            return jnp.where(m, 1.0, 0.0).astype(F32)

        m0 = ind(ids0 == me)
        m1 = ind(ids1 == me)
        n0 = ind(o0 == eidx)
        n1 = ind(o1 == eidx)
        stack = jnp.concatenate([m0, m1, n0, n1], axis=0).astype(BF16)
        tri = ind(lax.broadcasted_iota(jnp.int32, (tokens, tokens), 0) < lax.broadcasted_iota(jnp.int32, (tokens, tokens), 1)).astype(BF16)
        pre = jnp.dot(stack, tri, preferred_element_type=F32)
        s0, s1, r0, r1 = [pre[k * groups:(k + 1) * groups] for k in range(4)]
        c0 = jnp.sum(m0, axis=1, keepdims=True)
        c1 = jnp.sum(m1, axis=1, keepdims=True)
        k0 = jnp.sum(n0, axis=1, keepdims=True)
        run0 = jnp.zeros((1, 1), F32)
        run1 = jnp.zeros((1, 1), F32)
        b0 = []
        b1 = []
        for d in range(groups):
            b0.append(run0)
            b1.append(run1)
            run0 = run0 + c0[d:d + 1]
            run1 = run1 + c1[d:d + 1]
        before0 = jnp.concatenate(b0, axis=0)
        before1 = jnp.concatenate(b1, axis=0) + run0
        keep0 = jnp.logical_and(m0 > 0, before0 + s0 < cap)
        keep1 = jnp.logical_and(m1 > 0, before1 + s1 < cap)
        slot_tab[...] = jnp.where(keep0, s0, jnp.where(keep1, c0 + s1, -1.0))

        dmask = ind(eidx < me)
        g0 = []
        g1 = []
        for e in range(groups):
            a0 = ind(ids0 == e)
            a1 = ind(ids1 == e)
            g0.append(jnp.sum(jnp.sum(a0 * dmask, axis=1, keepdims=True), axis=0, keepdims=True))
            g1.append(jnp.sum(jnp.sum(a0 + a1 * dmask, axis=1, keepdims=True), axis=0, keepdims=True))
        own0 = jnp.logical_and(n0 > 0, jnp.concatenate(g0, axis=0) + r0 < cap)
        own1 = jnp.logical_and(n1 > 0, jnp.concatenate(g1, axis=0) + r1 < cap)
        slot_own = jnp.where(own0, r0, jnp.where(own1, k0 + r1, -1.0))
        gate_own = n0 * gates_ref[0:1, :] + n1 * gates_ref[1:2, :]
        both = jnp.concatenate([slot_own, gate_own, jnp.zeros((128 - 2 * groups, tokens), F32)], axis=0)
        comb_tab[...] = jnp.transpose(both)

        def stage_copy_own():
            return pltpu.make_async_copy(ostage, rbuf_ref.at[me], stsem)

        def stage_copy(t):
            return pltpu.make_async_copy(ostage, obuf_ref.at[tile_dev(t, 1)], stsem)

        def tile(t, carry):
            d = tile_dev(t, 1)

            @pl.when(t % 2 == 1)
            def _():
                wait_half(d, 0)
                wait_half(d, 1)

            def xcols(n):
                return pl.ds(pl.multiple_of(n * wchunk, 128), wchunk)

            def x_start(n):
                @pl.when(t == 0)
                def _():
                    pltpu.make_async_copy(x_ref.at[:, xcols(n)], xsrc.at[n % 2], xsem.at[n % 2]).start()

                @pl.when(t > 0)
                def _():
                    pltpu.make_async_copy(ag_ref.at[d, :, xcols(n)], xsrc.at[n % 2], xsem.at[n % 2]).start()

            x_start(0)
            row = slot_tab[pl.ds(d, 1), :]
            pbuf[...] = jnp.where(lax.broadcasted_iota(jnp.int32, (slots, tokens), 0).astype(F32) == row, 1.0, 0.0).astype(BF16)

            def gather(n, cc):
                @pl.when(n + 1 < ochunks)
                def _():
                    x_start(n + 1)
                pltpu.make_async_copy(x_ref.at[:, xcols(n)], xsrc.at[n % 2], xsem.at[n % 2]).wait()
                xg[:, xcols(n)] = jnp.dot(pbuf[...], xsrc[n % 2], preferred_element_type=F32).astype(BF16)
                return cc

            lax.fori_loop(0, ochunks, gather, 0)

            def up(i, cc):
                @pl.when(jnp.logical_and(t == 1, i == 0))
                def _():
                    wait_half(src_a, 0)
                    pass_a[0].start()

                @pl.when(jnp.logical_and(t == 1, i == 1))
                def _():
                    stage_copy_own().wait()

                @pl.when(jnp.logical_and(t > 1, i == 1))
                def _():
                    stage_copy(t - 1).wait()

                    @pl.when(t != 3)
                    def _():
                        ret_copy(t - 1).start()

                @pl.when(i + 1 < nfull)
                def _():
                    win_full(i + 1).start()

                @pl.when(i + 1 == nfull)
                def _():
                    win_tail.start()

                win_full(i).wait()
                pre_act = jnp.dot(xg[...], wbuf[i % 2], preferred_element_type=F32)
                hbuf[:, pl.ds(pl.multiple_of(i * wchunk, 128), wchunk)] = jax.nn.gelu(pre_act).astype(BF16)
                return cc

            lax.fori_loop(0, nfull, up, 0)
            win_tail.wait()

            @pl.when(t + 1 < groups)
            def _():
                win_full(0).start()
            pre_act = jnp.dot(xg[...], wbuf[nfull % 2, :, 0:tail], preferred_element_type=F32)
            hbuf[:, nfull * wchunk:hid] = jax.nn.gelu(pre_act).astype(BF16)

            def down(n, cc):
                @pl.when(t == 0)
                def _():
                    wout_part(n).wait()

                @pl.when(jnp.logical_and(t == 1, n == 1))
                def _():
                    wait_half(src_a, 1)
                    pass_a[1].start()
                    send_b[0].start()
                    send_b[1].start()

                @pl.when(jnp.logical_and(t == 2, n == 1))
                def _():
                    wait_half(src_b, 0)
                    pass_b[0].start()

                @pl.when(jnp.logical_and(t == 3, n == 0))
                def _():
                    wait_half(src_b, 1)
                    fwd_a.start()
                    fwd_b.start()
                    pass_b[1].start()
                    ret_copy(2).start()

                @pl.when(jnp.logical_and(t == 5, n == 0))
                def _():
                    wait_half(far, 0)
                    wait_half(far, 1)
                    pass_f[0].start()
                    pass_f[1].start()

                cols = pl.ds(pl.multiple_of(n * wchunk, 128), wchunk)
                ostage[:, cols] = jnp.dot(hbuf[...], wout[:, cols], preferred_element_type=F32).astype(BF16)
                return cc

            lax.fori_loop(0, ochunks, down, 0)

            @pl.when(t == 0)
            def _():
                stage_copy_own().start()

            @pl.when(t > 0)
            def _():
                stage_copy(t).start()
            return carry

        lax.fori_loop(0, groups, tile, 0)
        stage_copy(groups - 1).wait()
        ret_copy(groups - 1).start()

    def ids_ref_v(ref, d, j):
        return ref[pl.ds(d, 1), j, :]

    pl.run_scoped(
        compute,
        pltpu.VMEM((2, tokens, wchunk), BF16),
        pltpu.VMEM((slots, dim), BF16),
        pltpu.VMEM((slots, hid), BF16),
        pltpu.VMEM((2, dim, wchunk), BF16),
        pltpu.VMEM((hid, dim), BF16),
        pltpu.VMEM((slots, dim), BF16),
        pltpu.VMEM((slots, tokens), BF16),
        pltpu.SemaphoreType.DMA((2,)),
        pltpu.SemaphoreType.DMA((2,)),
        pltpu.SemaphoreType.DMA((ochunks,)),
        pltpu.SemaphoreType.DMA(()),
        pltpu.SemaphoreType.DMA(()),
    )

    def combine(acc, xb, rb, qbuf, xsem, rsem, osem):
        x_in = pltpu.make_async_copy(x_ref, xb, xsem)
        x_in.start()
        x_in.wait()
        for n in range(ochunks):
            cols = slice(n * wchunk, (n + 1) * wchunk)
            acc[:, cols] = xb[:, cols].astype(F32)

        def add_block(k, cc):
            e = comb_dev(k)

            @pl.when(k > 0)
            def _():
                remote(obuf_ref.at[e], rbuf_ref.at[e], ret_send.at[0], ret_recv.at[e], sib).wait_recv()
            cp = pltpu.make_async_copy(rbuf_ref.at[e], rb, rsem)
            cp.start()
            lane = lax.broadcasted_iota(jnp.int32, (tokens, 128), 1)
            tab = comb_tab[...]
            slot_col = jnp.sum(jnp.where(lane == e, tab, 0.0), axis=1, keepdims=True)
            gate_col = jnp.sum(jnp.where(lane == e + groups, tab, 0.0), axis=1, keepdims=True)
            qbuf[...] = jnp.where(lax.broadcasted_iota(jnp.int32, (tokens, slots), 1).astype(F32) == slot_col, 1.0, 0.0).astype(BF16)
            cp.wait()

            def part(n, c2):
                cols = pl.ds(pl.multiple_of(n * wchunk, 128), wchunk)
                pick = jnp.dot(qbuf[...], rb[:, cols], preferred_element_type=F32)
                acc[:, cols] = acc[:, cols] + gate_col * pick
                return c2

            return lax.fori_loop(0, ochunks, part, cc)

        lax.fori_loop(0, groups, add_block, 0)
        xb[...] = acc[...].astype(BF16)
        fin = pltpu.make_async_copy(xb, out_ref, osem)
        fin.start()
        fin.wait()

    pl.run_scoped(
        combine,
        pltpu.VMEM((tokens, dim), F32),
        pltpu.VMEM((tokens, dim), BF16),
        pltpu.VMEM((slots, dim), BF16),
        pltpu.VMEM((tokens, slots), BF16),
        pltpu.SemaphoreType.DMA(()),
        pltpu.SemaphoreType.DMA(()),
        pltpu.SemaphoreType.DMA(()),
    )

    for c in all_sends:
        c.wait_send()
    for t in range(1, groups):
        ret_copy(t).wait_send()


def solution(mesh):
    groups = mesh.shape["expert"]
    row_spec = P(("data", "expert"), None)
    weight_spec = P("expert", None, None)

    def device_step(token_rows, expert_ids, gate_weights, w_in, w_out):
        tokens, top_k = expert_ids.shape
        dim, hid = w_in.shape[1], w_in.shape[2]
        mean_load = tokens * top_k // groups
        slots = 7 * mean_load // 4
        cap = groups * mean_load
        any_spec = pl.BlockSpec(memory_space=pl.ANY)
        vmem_spec = pl.BlockSpec(memory_space=pltpu.VMEM)
        flops = 4 * groups * slots * dim * hid
        out = pl.pallas_call(
            functools.partial(layer_kernel, (groups, tokens, dim, hid, cap, slots)),
            out_shape=(
                jax.ShapeDtypeStruct((tokens, dim), BF16),
                jax.ShapeDtypeStruct((groups, tokens, dim), BF16),
                jax.ShapeDtypeStruct((groups, slots, dim), BF16),
                jax.ShapeDtypeStruct((groups, slots, dim), BF16),
            ),
            in_specs=[any_spec, any_spec, vmem_spec, any_spec, any_spec],
            out_specs=(any_spec, any_spec, any_spec, any_spec),
            scratch_shapes=[
                pltpu.VMEM((groups, top_k, tokens), jnp.int32),
                pltpu.VMEM((groups, tokens), F32),
                pltpu.VMEM((tokens, 128), F32),
                pltpu.SemaphoreType.DMA((groups,)),
                pltpu.SemaphoreType.DMA((groups,)),
                pltpu.SemaphoreType.DMA((16,)),
                pltpu.SemaphoreType.DMA((2 * groups,)),
                pltpu.SemaphoreType.DMA((groups,)),
                pltpu.SemaphoreType.DMA((groups,)),
            ],
            compiler_params=pltpu.CompilerParams(collective_id=0, has_side_effects=True, vmem_limit_bytes=67043328),
            cost_estimate=pl.CostEstimate(flops=flops, bytes_accessed=400000000, transcendentals=0),
            name="layer",
        )(token_rows, expert_ids.T, gate_weights.T, w_in.reshape(dim, hid), w_out.reshape(hid, dim))
        return out[0]

    return jax.shard_map(device_step, mesh=mesh, in_specs=(row_spec, row_spec, row_spec, weight_spec, weight_spec), out_specs=row_spec, check_vma=False)
```

```python
import functools

import jax
import jax.numpy as jnp
from jax import lax
from jax.experimental import pallas as pl
from jax.experimental.pallas import tpu as pltpu
from jax.sharding import PartitionSpec as P

MESH = pl.DeviceIdType.MESH
F32 = jnp.float32
BF16 = jnp.bfloat16


def layer_kernel(cfg, x_ref, ids_ref, gates_ref, win_ref, wout_ref, out_ref, ag_ref, obuf_ref, rbuf_ref,
                 ids_all, slot_tab, comb_tab, ids_send, ids_recv, ag_send, ag_recv, ret_send, ret_recv, barrier_unused=None):
    groups, tokens, dim, hid, cap, slots = cfg
    half = tokens // 2
    chips = groups // 2
    wchunk = 768
    nfull = hid // wchunk
    tail = hid - nfull * wchunk
    ochunks = dim // wchunk

    me = lax.axis_index("expert")
    chip = me // 2
    core = me % 2
    other = 1 - core
    sgn = 1 - 2 * core

    def dev(off, c):
        return ((chip + off + 2 * chips) % chips) * 2 + c

    sib = dev(0, other)
    src_a = dev(-sgn, core)
    src_b = dev(sgn, core)
    far = dev(2, core)

    def tile_dev(t, flip):
        q = t // 2
        p = t % 2
        f1 = q * (2 - q) * (3 - q) // 2
        f2 = q * (q - 1) * (3 - q) // 2
        f3 = q * (q - 1) * (q - 2) // 6
        off = flip * (f1 * (2 * p - 1) + f2 * (1 - 2 * p)) * sgn + 2 * f3
        c = core * (1 - p) + other * p
        return dev(off, c)

    def comb_dev(k):
        q = k // 2
        p = k % 2
        f1 = q * (2 - q) * (3 - q) // 2
        f2 = q * (q - 1) * (3 - q) // 2
        f3 = q * (q - 1) * (q - 2) // 6
        off = (f1 - f2) * sgn + 2 * f3
        c = core * (1 - p) + other * p
        return dev(off, c)

    def remote(src, dst, ssem, rsem, target):
        return pltpu.make_async_remote_copy(src_ref=src, dst_ref=dst, send_sem=ssem, recv_sem=rsem,
                                            device_id={"expert": target}, device_id_type=MESH)

    bar = pltpu.get_barrier_semaphore()
    for k in range(1, groups):
        pl.semaphore_signal(bar, inc=1, device_id={"expert": (me + k) % groups}, device_id_type=MESH)
    pl.semaphore_wait(bar, groups - 1)

    def ids_copy(k):
        return remote(ids_ref, ids_all.at[me], ids_send.at[k - 1], ids_recv.at[me], (me + k) % groups)

    def ag_copy(src, d, h, k, target):
        return remote(src, ag_ref.at[d, pl.ds(h * half, half)], ag_send.at[k], ag_recv.at[2 * d + h], target)

    def own_half(h):
        return x_ref.at[pl.ds(h * half, half)]

    def got_half(d, h):
        return ag_ref.at[d, pl.ds(h * half, half)]

    half_a = (1 - sgn) // 2
    half_b = 1 - half_a
    send_sib = [ag_copy(own_half(h), me, h, h, sib) for h in range(2)]
    send_a = [ag_copy(own_half(h), me, h, 2 + h, src_b) for h in range(2)]
    send_b1 = ag_copy(own_half(half_b), me, half_b, 4, src_a)
    send_b2 = ag_copy(own_half(half_a), me, half_a, 5, src_a)
    fwd_a = ag_copy(got_half(src_a, half_a), src_a, half_a, 6, src_b)
    fwd_b = ag_copy(got_half(src_b, half_b), src_b, half_b, 7, src_a)
    pass_a = [ag_copy(got_half(src_a, h), src_a, h, 8 + h, sib) for h in range(2)]
    pass_b1 = ag_copy(got_half(src_b, half_b), src_b, half_b, 10, sib)
    pass_b2 = ag_copy(got_half(src_b, half_a), src_b, half_a, 11, sib)
    pass_f1 = ag_copy(got_half(far, half_a), far, half_a, 12, sib)
    pass_f2 = ag_copy(got_half(far, half_b), far, half_b, 13, sib)
    all_sends = send_sib + send_a + [send_b1, send_b2, fwd_a, fwd_b] + pass_a + [pass_b1, pass_b2, pass_f1, pass_f2]

    def wait_half(d, h):
        ag_copy(got_half(d, h), d, h, 0, sib).wait_recv()

    def ret_copy(t):
        d = tile_dev(t, 1)
        return remote(obuf_ref.at[d], rbuf_ref.at[me], ret_send.at[t], ret_recv.at[me], d)

    for k in range(1, groups):
        ids_copy(k).start()
    for c in send_sib + send_a:
        c.start()

    def compute(xsrc, xg, hbuf, pact, wbuf, wout, ostage, pbuf, xsem, wsem, osem, stsem, isem):
        own_ids = pltpu.make_async_copy(ids_ref, ids_all.at[me], isem)
        own_ids.start()

        def win_full(i):
            return pltpu.make_async_copy(win_ref.at[:, pl.ds(pl.multiple_of(i * wchunk, 128), wchunk)], wbuf.at[i % 2], wsem.at[i % 2])

        win_tail = pltpu.make_async_copy(win_ref.at[:, pl.ds(nfull * wchunk, tail)], wbuf.at[nfull % 2, :, pl.ds(0, tail)], wsem.at[nfull % 2])

        def wout_part(n):
            return pltpu.make_async_copy(wout_ref.at[:, pl.ds(pl.multiple_of(n * wchunk, 128), wchunk)], wout.at[:, pl.ds(pl.multiple_of(n * wchunk, 128), wchunk)], osem.at[n])

        win_full(0).start()
        for n in range(ochunks):
            wout_part(n).start()

        own_ids.wait()
        for k in range(1, groups):
            ids_copy(k).wait_send()
        for k in range(1, groups):
            d = (me + k) % groups
            remote(ids_ref, ids_all.at[d], ids_send.at[0], ids_recv.at[d], sib).wait_recv()
        ids0 = ids_all[:, 0, :]
        ids1 = ids_all[:, 1, :]
        o0 = ids_ref_v(ids_all, me, 0)
        o1 = ids_ref_v(ids_all, me, 1)
        eidx = lax.broadcasted_iota(jnp.int32, (groups, tokens), 0)

        def ind(m):
            return jnp.where(m, 1.0, 0.0).astype(F32)

        m0 = ind(ids0 == me)
        m1 = ind(ids1 == me)
        n0 = ind(o0 == eidx)
        n1 = ind(o1 == eidx)
        stack = jnp.concatenate([m0, m1, n0, n1], axis=0).astype(BF16)
        tri = ind(lax.broadcasted_iota(jnp.int32, (tokens, tokens), 0) < lax.broadcasted_iota(jnp.int32, (tokens, tokens), 1)).astype(BF16)
        pre = jnp.dot(stack, tri, preferred_element_type=F32)
        s0, s1, r0, r1 = [pre[k * groups:(k + 1) * groups] for k in range(4)]
        c0 = jnp.sum(m0, axis=1, keepdims=True)
        c1 = jnp.sum(m1, axis=1, keepdims=True)
        k0 = jnp.sum(n0, axis=1, keepdims=True)
        run0 = jnp.zeros((1, 1), F32)
        run1 = jnp.zeros((1, 1), F32)
        b0 = []
        b1 = []
        for d in range(groups):
            b0.append(run0)
            b1.append(run1)
            run0 = run0 + c0[d:d + 1]
            run1 = run1 + c1[d:d + 1]
        before0 = jnp.concatenate(b0, axis=0)
        before1 = jnp.concatenate(b1, axis=0) + run0
        keep0 = jnp.logical_and(m0 > 0, before0 + s0 < cap)
        keep1 = jnp.logical_and(m1 > 0, before1 + s1 < cap)
        slot_tab[...] = jnp.where(keep0, s0, jnp.where(keep1, c0 + s1, -1.0))

        dmask = ind(eidx < me)
        g0 = []
        g1 = []
        for e in range(groups):
            a0 = ind(ids0 == e)
            a1 = ind(ids1 == e)
            g0.append(jnp.sum(jnp.sum(a0 * dmask, axis=1, keepdims=True), axis=0, keepdims=True))
            g1.append(jnp.sum(jnp.sum(a0 + a1 * dmask, axis=1, keepdims=True), axis=0, keepdims=True))
        own0 = jnp.logical_and(n0 > 0, jnp.concatenate(g0, axis=0) + r0 < cap)
        own1 = jnp.logical_and(n1 > 0, jnp.concatenate(g1, axis=0) + r1 < cap)
        slot_own = jnp.where(own0, r0, jnp.where(own1, k0 + r1, -1.0))
        gate_own = n0 * gates_ref[0:1, :] + n1 * gates_ref[1:2, :]
        both = jnp.concatenate([slot_own, gate_own, jnp.zeros((128 - 2 * groups, tokens), F32)], axis=0)
        comb_tab[...] = jnp.transpose(both)

        def stage_copy_own():
            return pltpu.make_async_copy(ostage, rbuf_ref.at[me], stsem)

        def stage_copy(t):
            return pltpu.make_async_copy(ostage, obuf_ref.at[tile_dev(t, 1)], stsem)

        def tile(t, carry):
            d = tile_dev(t, 1)

            @pl.when(t % 2 == 1)
            def _():
                wait_half(d, 0)
                wait_half(d, 1)

            def xcols(n):
                return pl.ds(pl.multiple_of(n * wchunk, 128), wchunk)

            def x_start(n):
                @pl.when(t == 0)
                def _():
                    pltpu.make_async_copy(x_ref.at[:, xcols(n)], xsrc.at[n % 2], xsem.at[n % 2]).start()

                @pl.when(t > 0)
                def _():
                    pltpu.make_async_copy(ag_ref.at[d, :, xcols(n)], xsrc.at[n % 2], xsem.at[n % 2]).start()

            x_start(0)
            row = slot_tab[pl.ds(d, 1), :]
            pbuf[...] = jnp.where(lax.broadcasted_iota(jnp.int32, (slots, tokens), 0).astype(F32) == row, 1.0, 0.0).astype(BF16)

            def gather(n, cc):
                @pl.when(n + 1 < ochunks)
                def _():
                    x_start(n + 1)
                pltpu.make_async_copy(x_ref.at[:, xcols(n)], xsrc.at[n % 2], xsem.at[n % 2]).wait()
                xg[:, xcols(n)] = jnp.dot(pbuf[...], xsrc[n % 2], preferred_element_type=F32).astype(BF16)
                return cc

            lax.fori_loop(0, ochunks, gather, 0)

            def up(i, cc):
                @pl.when(jnp.logical_and(t == 1, i == 2))
                def _():
                    stage_copy_own().wait()
                    wait_half(src_a, 0)
                    pass_a[0].start()

                @pl.when(jnp.logical_and(t == 3, i == 3))
                def _():
                    wait_half(src_b, half_b)
                    fwd_b.start()
                    pass_b1.start()

                @pl.when(jnp.logical_and(t == 4, i == 3))
                def _():
                    wait_half(far, half_a)
                    pass_f1.start()

                @pl.when(jnp.logical_and(t > 1, i == 1))
                def _():
                    stage_copy(t - 1).wait()

                    @pl.when(t != 3)
                    def _():
                        ret_copy(t - 1).start()

                @pl.when(i + 1 < nfull)
                def _():
                    win_full(i + 1).start()

                @pl.when(i + 1 == nfull)
                def _():
                    win_tail.start()

                win_full(i).wait()
                prev = pl.ds(pl.multiple_of((i - 1) * wchunk, 128), wchunk)
                hbuf[:, prev] = jax.nn.gelu(pact[(i - 1) % 2]).astype(BF16)
                pact[i % 2] = jnp.dot(xg[...], wbuf[i % 2], preferred_element_type=F32)
                return cc

            win_full(1).start()
            win_full(0).wait()
            pact[0] = jnp.dot(xg[...], wbuf[0], preferred_element_type=F32)
            lax.fori_loop(1, nfull, up, 0)
            win_tail.wait()

            @pl.when(t + 1 < groups)
            def _():
                win_full(0).start()
            hbuf[:, (nfull - 1) * wchunk:nfull * wchunk] = jax.nn.gelu(pact[(nfull - 1) % 2]).astype(BF16)
            pre_act = jnp.dot(xg[...], wbuf[nfull % 2, :, 0:tail], preferred_element_type=F32)
            hbuf[:, nfull * wchunk:hid] = jax.nn.gelu(pre_act).astype(BF16)

            def down(n, cc):
                @pl.when(t == 0)
                def _():
                    wout_part(n).wait()

                @pl.when(jnp.logical_and(t == 1, n == 0))
                def _():
                    send_b1.start()
                    send_b2.start()
                    wait_half(src_a, 1)
                    fwd_a.start()
                    pass_a[1].start()

                @pl.when(jnp.logical_and(t == 3, n == 2))
                def _():
                    wait_half(src_b, half_a)
                    pass_b2.start()
                    ret_copy(2).start()

                @pl.when(jnp.logical_and(t == 5, n == 0))
                def _():
                    wait_half(far, half_b)
                    pass_f2.start()

                cols = pl.ds(pl.multiple_of(n * wchunk, 128), wchunk)
                ostage[:, cols] = jnp.dot(hbuf[...], wout[:, cols], preferred_element_type=F32).astype(BF16)
                return cc

            lax.fori_loop(0, ochunks, down, 0)

            @pl.when(t == 0)
            def _():
                stage_copy_own().start()

            @pl.when(t > 0)
            def _():
                stage_copy(t).start()
            return carry

        lax.fori_loop(0, groups, tile, 0)
        stage_copy(groups - 1).wait()
        ret_copy(groups - 1).start()

    def ids_ref_v(ref, d, j):
        return ref[pl.ds(d, 1), j, :]

    pl.run_scoped(
        compute,
        pltpu.VMEM((2, tokens, wchunk), BF16),
        pltpu.VMEM((slots, dim), BF16),
        pltpu.VMEM((slots, hid), BF16),
        pltpu.VMEM((2, slots, wchunk), F32),
        pltpu.VMEM((2, dim, wchunk), BF16),
        pltpu.VMEM((hid, dim), BF16),
        pltpu.VMEM((slots, dim), BF16),
        pltpu.VMEM((slots, tokens), BF16),
        pltpu.SemaphoreType.DMA((2,)),
        pltpu.SemaphoreType.DMA((2,)),
        pltpu.SemaphoreType.DMA((ochunks,)),
        pltpu.SemaphoreType.DMA(()),
        pltpu.SemaphoreType.DMA(()),
    )

    def combine(acc, xb, rb, qbuf, xsem, rsem, osem):
        x_in = pltpu.make_async_copy(x_ref, xb, xsem)
        x_in.start()
        x_in.wait()
        for n in range(ochunks):
            cols = slice(n * wchunk, (n + 1) * wchunk)
            acc[:, cols] = xb[:, cols].astype(F32)

        def block_copy(k):
            return pltpu.make_async_copy(rbuf_ref.at[comb_dev(k)], rb.at[k % 2], rsem.at[k % 2])

        def block_ready(k):
            e = comb_dev(k)
            remote(obuf_ref.at[e], rbuf_ref.at[e], ret_send.at[0], ret_recv.at[e], sib).wait_recv()
            block_copy(k).start()

        block_copy(0).start()

        def add_block(k, cc):
            e = comb_dev(k)

            @pl.when(k < groups - 2)
            def _():
                block_ready(k + 1)
            lane = lax.broadcasted_iota(jnp.int32, (tokens, 128), 1)
            tab = comb_tab[...]
            slot_col = jnp.sum(jnp.where(lane == e, tab, 0.0), axis=1, keepdims=True)
            gate_col = jnp.sum(jnp.where(lane == e + groups, tab, 0.0), axis=1, keepdims=True)
            qbuf[...] = jnp.where(lax.broadcasted_iota(jnp.int32, (tokens, slots), 1).astype(F32) == slot_col, 1.0, 0.0).astype(BF16)
            block_copy(k).wait()

            def part(n, c2):
                cols = pl.ds(pl.multiple_of(n * wchunk, 128), wchunk)
                pick = jnp.dot(qbuf[...], rb[k % 2, :, cols], preferred_element_type=F32)
                acc[:, cols] = acc[:, cols] + gate_col * pick
                return c2

            lax.fori_loop(0, ochunks, part, 0)

            @pl.when(k == groups - 2)
            def _():
                block_ready(k + 1)
            return cc

        lax.fori_loop(0, groups, add_block, 0)
        xb[...] = acc[...].astype(BF16)
        fin = pltpu.make_async_copy(xb, out_ref, osem)
        fin.start()
        fin.wait()

    pl.run_scoped(
        combine,
        pltpu.VMEM((tokens, dim), F32),
        pltpu.VMEM((tokens, dim), BF16),
        pltpu.VMEM((2, slots, dim), BF16),
        pltpu.VMEM((tokens, slots), BF16),
        pltpu.SemaphoreType.DMA(()),
        pltpu.SemaphoreType.DMA((2,)),
        pltpu.SemaphoreType.DMA(()),
    )

    for c in all_sends:
        c.wait_send()
    for t in range(1, groups):
        ret_copy(t).wait_send()


def solution(mesh):
    groups = mesh.shape["expert"]
    row_spec = P(("data", "expert"), None)
    weight_spec = P("expert", None, None)

    def device_step(token_rows, expert_ids, gate_weights, w_in, w_out):
        tokens, top_k = expert_ids.shape
        dim, hid = w_in.shape[1], w_in.shape[2]
        mean_load = tokens * top_k // groups
        slots = 7 * mean_load // 4
        cap = groups * mean_load
        any_spec = pl.BlockSpec(memory_space=pl.ANY)
        vmem_spec = pl.BlockSpec(memory_space=pltpu.VMEM)
        flops = 4 * groups * slots * dim * hid
        out = pl.pallas_call(
            functools.partial(layer_kernel, (groups, tokens, dim, hid, cap, slots)),
            out_shape=(
                jax.ShapeDtypeStruct((tokens, dim), BF16),
                jax.ShapeDtypeStruct((groups, tokens, dim), BF16),
                jax.ShapeDtypeStruct((groups, slots, dim), BF16),
                jax.ShapeDtypeStruct((groups, slots, dim), BF16),
            ),
            in_specs=[any_spec, any_spec, vmem_spec, any_spec, any_spec],
            out_specs=(any_spec, any_spec, any_spec, any_spec),
            scratch_shapes=[
                pltpu.VMEM((groups, top_k, tokens), jnp.int32),
                pltpu.VMEM((groups, tokens), F32),
                pltpu.VMEM((tokens, 128), F32),
                pltpu.SemaphoreType.DMA((groups,)),
                pltpu.SemaphoreType.DMA((groups,)),
                pltpu.SemaphoreType.DMA((16,)),
                pltpu.SemaphoreType.DMA((2 * groups,)),
                pltpu.SemaphoreType.DMA((groups,)),
                pltpu.SemaphoreType.DMA((groups,)),
            ],
            compiler_params=pltpu.CompilerParams(collective_id=0, has_side_effects=True, vmem_limit_bytes=67043328),
            cost_estimate=pl.CostEstimate(flops=flops, bytes_accessed=400000000, transcendentals=0),
            name="layer",
        )(token_rows, expert_ids.T, gate_weights.T, w_in.reshape(dim, hid), w_out.reshape(hid, dim))
        return out[0]

    return jax.shard_map(device_step, mesh=mesh, in_specs=(row_spec, row_spec, row_spec, weight_spec, weight_spec), out_specs=row_spec, check_vma=False)
```

```python
import functools

import jax
import jax.numpy as jnp
from jax import lax
from jax.experimental import pallas as pl
from jax.experimental.pallas import tpu as pltpu
from jax.sharding import PartitionSpec as P

MESH = pl.DeviceIdType.MESH
F32 = jnp.float32
BF16 = jnp.bfloat16


def layer_kernel(cfg, x_ref, ids_ref, gates_ref, win_ref, wout_ref, acc_ref, tab_ref, rfar_ref, ag_ref, obuf_ref, rbuf_ref,
                 ids_all, slot_tab, comb_tab, ids_send, ids_recv, ag_send, ag_recv, ret_send, ret_recv):
    groups, tokens, dim, hid, cap, slots = cfg
    half = tokens // 2
    chips = groups // 2
    wchunk = 768
    nfull = hid // wchunk
    tail = hid - nfull * wchunk
    ochunks = dim // wchunk

    me = lax.axis_index("expert")
    chip = me // 2
    core = me % 2
    other = 1 - core
    sgn = 1 - 2 * core

    def dev(off, c):
        return ((chip + off + 2 * chips) % chips) * 2 + c

    sib = dev(0, other)
    src_a = dev(-sgn, core)
    src_b = dev(sgn, core)
    far = dev(2, core)

    def tile_dev(t, flip):
        q = t // 2
        p = t % 2
        f1 = q * (2 - q) * (3 - q) // 2
        f2 = q * (q - 1) * (3 - q) // 2
        f3 = q * (q - 1) * (q - 2) // 6
        off = flip * (f1 * (2 * p - 1) + f2 * (1 - 2 * p)) * sgn + 2 * f3
        c = core * (1 - p) + other * p
        return dev(off, c)

    def comb_dev(k):
        q = k // 2
        p = k % 2
        f1 = q * (2 - q) * (3 - q) // 2
        f2 = q * (q - 1) * (3 - q) // 2
        f3 = q * (q - 1) * (q - 2) // 6
        off = (f1 - f2) * sgn + 2 * f3
        c = core * (1 - p) + other * p
        return dev(off, c)

    def remote(src, dst, ssem, rsem, target):
        return pltpu.make_async_remote_copy(src_ref=src, dst_ref=dst, send_sem=ssem, recv_sem=rsem,
                                            device_id={"expert": target}, device_id_type=MESH)

    bar = pltpu.get_barrier_semaphore()
    for k in range(1, groups):
        pl.semaphore_signal(bar, inc=1, device_id={"expert": (me + k) % groups}, device_id_type=MESH)
    pl.semaphore_wait(bar, groups - 1)

    def ids_copy(k):
        return remote(ids_ref, ids_all.at[me], ids_send.at[k - 1], ids_recv.at[me], (me + k) % groups)

    def ag_copy(src, d, h, k, target):
        return remote(src, ag_ref.at[d, pl.ds(h * half, half)], ag_send.at[k], ag_recv.at[2 * d + h], target)

    def own_half(h):
        return x_ref.at[pl.ds(h * half, half)]

    def got_half(d, h):
        return ag_ref.at[d, pl.ds(h * half, half)]

    half_a = (1 - sgn) // 2
    half_b = 1 - half_a
    send_sib = [ag_copy(own_half(h), me, h, h, sib) for h in range(2)]
    send_a = [ag_copy(own_half(h), me, h, 2 + h, src_b) for h in range(2)]
    send_b1 = ag_copy(own_half(half_b), me, half_b, 4, src_a)
    send_b2 = ag_copy(own_half(half_a), me, half_a, 5, src_a)
    fwd_a = ag_copy(got_half(src_a, half_a), src_a, half_a, 6, src_b)
    fwd_b = ag_copy(got_half(src_b, half_b), src_b, half_b, 7, src_a)
    pass_a = [ag_copy(got_half(src_a, h), src_a, h, 8 + h, sib) for h in range(2)]
    pass_b1 = ag_copy(got_half(src_b, half_b), src_b, half_b, 10, sib)
    pass_b2 = ag_copy(got_half(src_b, half_a), src_b, half_a, 11, sib)
    pass_f1 = ag_copy(got_half(far, half_a), far, half_a, 12, sib)
    pass_f2 = ag_copy(got_half(far, half_b), far, half_b, 13, sib)
    all_sends = send_sib + send_a + [send_b1, send_b2, fwd_a, fwd_b] + pass_a + [pass_b1, pass_b2, pass_f1, pass_f2]

    def wait_half(d, h):
        ag_copy(got_half(d, h), d, h, 0, sib).wait_recv()

    def ret_copy(t):
        d = tile_dev(t, 1)
        return remote(obuf_ref.at[d], rbuf_ref.at[me], ret_send.at[t], ret_recv.at[me], d)

    def ret_far(p):
        d = dev(2, core * (1 - p) + other * p)
        return remote(obuf_ref.at[d], rfar_ref.at[core], ret_send.at[groups - 2 + p], ret_recv.at[me], d)

    for k in range(1, groups):
        ids_copy(k).start()
    for c in send_sib + send_a:
        c.start()

    def compute(xsrc, xg, hbuf, pact, wbuf, wout, pbuf, xsem, wsem, osem, stsem, isem):
        passes = groups // 2
        ochunk = 512
        ofull = dim // ochunk
        otail = dim - ofull * ochunk
        own_ids = pltpu.make_async_copy(ids_ref, ids_all.at[me], isem)
        own_ids.start()

        def win_full(i):
            return pltpu.make_async_copy(win_ref.at[:, pl.ds(pl.multiple_of(i * wchunk, 128), wchunk)], wbuf.at[i % 2], wsem.at[i % 2])

        win_tail = pltpu.make_async_copy(win_ref.at[:, pl.ds(nfull * wchunk, tail)], wbuf.at[nfull % 2, :, pl.ds(0, tail)], wsem.at[nfull % 2])

        def wout_part(n, g):
            return pltpu.make_async_copy(wout_ref.at[:, pl.ds(pl.multiple_of(n * ochunk, 128), ochunk)], wout.at[g % 2], osem.at[g % 2])

        def wout_tail(g):
            return pltpu.make_async_copy(wout_ref.at[:, pl.ds(ofull * ochunk, otail)], wout.at[g % 2, :, pl.ds(0, otail)], osem.at[g % 2])

        win_full(0).start()
        wout_part(0, 0).start()

        own_ids.wait()
        for k in range(1, groups):
            ids_copy(k).wait_send()
        for k in range(1, groups):
            d = (me + k) % groups
            remote(ids_ref, ids_all.at[d], ids_send.at[0], ids_recv.at[d], sib).wait_recv()
        ids0 = ids_all[:, 0, :]
        ids1 = ids_all[:, 1, :]
        o0 = ids_ref_v(ids_all, me, 0)
        o1 = ids_ref_v(ids_all, me, 1)
        eidx = lax.broadcasted_iota(jnp.int32, (groups, tokens), 0)

        def ind(m):
            return jnp.where(m, 1.0, 0.0).astype(F32)

        m0 = ind(ids0 == me)
        m1 = ind(ids1 == me)
        n0 = ind(o0 == eidx)
        n1 = ind(o1 == eidx)
        stack = jnp.concatenate([m0, m1, n0, n1], axis=0).astype(BF16)
        parts = []
        for h in range(2):
            earlier = lax.broadcasted_iota(jnp.int32, (tokens, half), 0) < lax.broadcasted_iota(jnp.int32, (tokens, half), 1) + h * half
            xsrc[h, :, 0:half] = ind(earlier).astype(BF16)
            parts.append(jnp.dot(stack, xsrc[h, :, 0:half], preferred_element_type=F32))
        pre = jnp.concatenate(parts, axis=1)
        s0, s1, r0, r1 = [pre[k * groups:(k + 1) * groups] for k in range(4)]
        c0 = jnp.sum(m0, axis=1, keepdims=True)
        c1 = jnp.sum(m1, axis=1, keepdims=True)
        k0 = jnp.sum(n0, axis=1, keepdims=True)
        run0 = jnp.zeros((1, 1), F32)
        run1 = jnp.zeros((1, 1), F32)
        b0 = []
        b1 = []
        for d in range(groups):
            b0.append(run0)
            b1.append(run1)
            run0 = run0 + c0[d:d + 1]
            run1 = run1 + c1[d:d + 1]
        before0 = jnp.concatenate(b0, axis=0)
        before1 = jnp.concatenate(b1, axis=0) + run0
        keep0 = jnp.logical_and(m0 > 0, before0 + s0 < cap)
        keep1 = jnp.logical_and(m1 > 0, before1 + s1 < cap)
        slot_tab[...] = jnp.where(keep0, s0, jnp.where(keep1, c0 + s1, -1.0))

        dmask = ind(eidx < me)
        g0 = []
        g1 = []
        for e in range(groups):
            a0 = ind(ids0 == e)
            a1 = ind(ids1 == e)
            g0.append(jnp.sum(jnp.sum(a0 * dmask, axis=1, keepdims=True), axis=0, keepdims=True))
            g1.append(jnp.sum(jnp.sum(a0 + a1 * dmask, axis=1, keepdims=True), axis=0, keepdims=True))
        own0 = jnp.logical_and(n0 > 0, jnp.concatenate(g0, axis=0) + r0 < cap)
        own1 = jnp.logical_and(n1 > 0, jnp.concatenate(g1, axis=0) + r1 < cap)
        slot_own = jnp.where(own0, r0, jnp.where(own1, k0 + r1, -1.0))
        gate_own = n0 * gates_ref[0:1, :] + n1 * gates_ref[1:2, :]
        far_rows = []
        for v in (slot_own, gate_own):
            for b in range(2):
                far_rows.append(jnp.sum(jnp.where(eidx == dev(2, b), v, 0.0), axis=0, keepdims=True))
        both = jnp.concatenate([slot_own, gate_own] + far_rows + [jnp.zeros((124 - 2 * groups, tokens), F32)], axis=0)
        comb_tab[...] = jnp.transpose(both)

        def stage_rows(p):
            return xg.at[pl.ds(p * slots, slots)]

        def stage_own():
            return pltpu.make_async_copy(stage_rows(0), rbuf_ref.at[me], stsem.at[0])

        def stage_copy(q, p):
            return pltpu.make_async_copy(stage_rows(p), obuf_ref.at[tile_dev(2 * q + p, 1)], stsem.at[p])

        def xcols(n):
            return pl.ds(pl.multiple_of(n * wchunk, 128), wchunk)

        def one_pass(q, carry):
            wait_half(tile_dev(2 * q + 1, 1), 0)
            wait_half(tile_dev(2 * q + 1, 1), 1)

            def x_start(m):
                p = m // ochunks
                n = m % ochunks
                own = jnp.logical_and(q == 0, p == 0)

                @pl.when(own)
                def _():
                    pltpu.make_async_copy(x_ref.at[:, xcols(n)], xsrc.at[m % 2], xsem.at[m % 2]).start()

                @pl.when(jnp.logical_not(own))
                def _():
                    pltpu.make_async_copy(ag_ref.at[tile_dev(2 * q + p, 1), :, xcols(n)], xsrc.at[m % 2], xsem.at[m % 2]).start()

            x_start(0)

            @pl.when(q == 1)
            def _():
                stage_own().wait()

            @pl.when(q > 1)
            def _():
                stage_copy(q - 1, 0).wait()
                ret_copy(2 * q - 2).start()

            @pl.when(q > 0)
            def _():
                stage_copy(q - 1, 1).wait()
                ret_copy(2 * q - 1).start()

            def gather_block(p, c1):
                row = slot_tab[pl.ds(tile_dev(2 * q + p, 1), 1), :]
                pbuf[...] = jnp.where(lax.broadcasted_iota(jnp.int32, (slots, tokens), 0).astype(F32) == row, 1.0, 0.0).astype(BF16)
                rows = pl.ds(pl.multiple_of(p * slots, slots), slots)

                def gather(n, c2):
                    m = p * ochunks + n

                    @pl.when(m + 1 < 2 * ochunks)
                    def _():
                        x_start(m + 1)
                    pltpu.make_async_copy(x_ref.at[:, xcols(n)], xsrc.at[m % 2], xsem.at[m % 2]).wait()
                    xg[rows, xcols(n)] = jnp.dot(pbuf[...], xsrc[m % 2], preferred_element_type=F32).astype(BF16)
                    return c2

                return lax.fori_loop(0, ochunks, gather, c1)

            lax.fori_loop(0, 2, gather_block, 0)

            def up(i, cc):
                @pl.when(i + 1 < nfull)
                def _():
                    win_full(i + 1).start()

                @pl.when(i + 1 == nfull)
                def _():
                    win_tail.start()

                win_full(i).wait()
                hbuf[:, xcols(i - 1)] = jax.nn.gelu(pact[...]).astype(BF16)
                pact[...] = jnp.dot(xg[...], wbuf[i % 2], preferred_element_type=F32)
                return cc

            win_full(1).start()
            win_full(0).wait()
            pact[...] = jnp.dot(xg[...], wbuf[0], preferred_element_type=F32)
            lax.fori_loop(1, nfull, up, 0)
            win_tail.wait()

            @pl.when(q + 1 < passes)
            def _():
                win_full(0).start()
            hbuf[:, (nfull - 1) * wchunk:nfull * wchunk] = jax.nn.gelu(pact[...]).astype(BF16)
            pre_act = jnp.dot(xg[...], wbuf[nfull % 2, :, 0:tail], preferred_element_type=F32)
            hbuf[:, nfull * wchunk:hid] = jax.nn.gelu(pre_act).astype(BF16)

            def down(n, cc):
                g = q * (ofull + 1) + n

                @pl.when(n + 1 < ofull)
                def _():
                    wout_part(n + 1, g + 1).start()

                @pl.when(n + 1 == ofull)
                def _():
                    wout_tail(g + 1).start()

                @pl.when(jnp.logical_and(q == 0, n == 0))
                def _():
                    wait_half(src_a, 0)
                    pass_a[0].start()

                @pl.when(jnp.logical_and(q == 0, n == 3))
                def _():
                    send_b1.start()
                    send_b2.start()
                    wait_half(src_a, 1)
                    pass_a[1].start()

                @pl.when(jnp.logical_and(q == 1, n == 0))
                def _():
                    wait_half(src_b, half_b)
                    pass_b1.start()

                @pl.when(jnp.logical_and(q == 1, n == 2))
                def _():
                    fwd_a.start()
                    fwd_b.start()

                @pl.when(jnp.logical_and(q == 1, n == 3))
                def _():
                    wait_half(src_b, half_a)
                    pass_b2.start()

                @pl.when(jnp.logical_and(q == 2, n == 3))
                def _():
                    wait_half(far, half_a)
                    pass_f1.start()
                    wait_half(far, half_b)
                    pass_f2.start()

                wout_part(n, g).wait()

                def block(p, c2):
                    rows = pl.ds(pl.multiple_of(p * slots, slots), slots)
                    xg[rows, pl.ds(pl.multiple_of(n * ochunk, 128), ochunk)] = jnp.dot(hbuf[rows, :], wout[g % 2], preferred_element_type=F32).astype(BF16)
                    return c2

                return lax.fori_loop(0, 2, block, cc)

            lax.fori_loop(0, ofull, down, 0)
            last = q * (ofull + 1) + ofull

            @pl.when(q + 1 < passes)
            def _():
                wout_part(0, last + 1).start()
            wout_tail(last).wait()

            def block_tail(p, c2):
                rows = pl.ds(pl.multiple_of(p * slots, slots), slots)
                xg[rows, ofull * ochunk:dim] = jnp.dot(hbuf[rows, :], wout[last % 2, :, 0:otail], preferred_element_type=F32).astype(BF16)
                return c2

            lax.fori_loop(0, 2, block_tail, 0)

            @pl.when(q == 0)
            def _():
                stage_own().start()

            @pl.when(q > 0)
            def _():
                stage_copy(q, 0).start()
            stage_copy(q, 1).start()
            return carry

        lax.fori_loop(0, passes, one_pass, 0)
        for p in range(2):
            stage_copy(passes - 1, p).wait()
            ret_far(p).start()

    def ids_ref_v(ref, d, j):
        return ref[pl.ds(d, 1), j, :]

    pl.run_scoped(
        compute,
        pltpu.VMEM((2, tokens, wchunk), BF16),
        pltpu.VMEM((2 * slots, dim), BF16),
        pltpu.VMEM((2 * slots, hid), BF16),
        pltpu.VMEM((2 * slots, wchunk), F32),
        pltpu.VMEM((2, dim, wchunk), BF16),
        pltpu.VMEM((2, hid, 512), BF16),
        pltpu.VMEM((slots, tokens), BF16),
        pltpu.SemaphoreType.DMA((2,)),
        pltpu.SemaphoreType.DMA((2,)),
        pltpu.SemaphoreType.DMA((2,)),
        pltpu.SemaphoreType.DMA((2,)),
        pltpu.SemaphoreType.DMA(()),
    )

    def combine(acc, xb, rb, qbuf, xsem, rsem, osem):
        near = groups - 2
        tab_out = pltpu.make_async_copy(comb_tab, tab_ref, osem.at[1])
        tab_out.start()
        x_in = pltpu.make_async_copy(x_ref, xb, xsem)
        x_in.start()
        x_in.wait()
        for n in range(ochunks):
            cols = slice(n * wchunk, (n + 1) * wchunk)
            acc[:, cols] = xb[:, cols].astype(F32)

        def block_copy(k):
            return pltpu.make_async_copy(rbuf_ref.at[comb_dev(k)], rb.at[k % 2], rsem.at[k % 2])

        def block_ready(k):
            e = comb_dev(k)
            remote(obuf_ref.at[e], rbuf_ref.at[e], ret_send.at[0], ret_recv.at[e], sib).wait_recv()
            block_copy(k).start()

        block_copy(0).start()

        def add_block(k, cc):
            e = comb_dev(k)

            @pl.when(k + 1 < near)
            def _():
                block_ready(k + 1)
            lane = lax.broadcasted_iota(jnp.int32, (tokens, 128), 1)
            tab = comb_tab[...]
            slot_col = jnp.sum(jnp.where(lane == e, tab, 0.0), axis=1, keepdims=True)
            gate_col = jnp.sum(jnp.where(lane == e + groups, tab, 0.0), axis=1, keepdims=True)
            qbuf[...] = jnp.where(lax.broadcasted_iota(jnp.int32, (tokens, slots), 1).astype(F32) == slot_col, 1.0, 0.0).astype(BF16)
            block_copy(k).wait()

            def part(n, c2):
                cols = pl.ds(pl.multiple_of(n * wchunk, 128), wchunk)
                pick = jnp.dot(qbuf[...], rb[k % 2, :, cols], preferred_element_type=F32)
                acc[:, cols] = acc[:, cols] + gate_col * pick
                return c2

            return lax.fori_loop(0, ochunks, part, cc)

        lax.fori_loop(0, near, add_block, 0)
        fin = pltpu.make_async_copy(acc, acc_ref, osem.at[0])
        fin.start()
        fin.wait()
        tab_out.wait()

    pl.run_scoped(
        combine,
        pltpu.VMEM((tokens, dim), F32),
        pltpu.VMEM((tokens, dim), BF16),
        pltpu.VMEM((2, slots, dim), BF16),
        pltpu.VMEM((tokens, slots), BF16),
        pltpu.SemaphoreType.DMA(()),
        pltpu.SemaphoreType.DMA((2,)),
        pltpu.SemaphoreType.DMA((2,)),
    )

    for c in all_sends:
        c.wait_send()
    for t in range(1, groups - 2):
        ret_copy(t).wait_send()
    for p in range(2):
        ret_far(p).wait_send()
        remote(obuf_ref.at[me], rfar_ref.at[p], ret_send.at[0], ret_recv.at[dev(2, p)], sib).wait_recv()


def finish_kernel(base, acc_ref, tab_ref, rfar_ref, out_ref):
    rows, dim = out_ref.shape
    slots = rfar_ref.shape[1]
    total = acc_ref[...]
    col = lax.broadcasted_iota(jnp.int32, (rows, slots), 1).astype(F32)
    for b in range(2):
        pick = jnp.where(col == tab_ref[:, base + b:base + b + 1], 1.0, 0.0).astype(BF16)
        total = total + tab_ref[:, base + 2 + b:base + 3 + b] * jnp.dot(pick, rfar_ref[b], preferred_element_type=F32)
    out_ref[...] = total.astype(BF16)


def solution(mesh):
    groups = mesh.shape["expert"]
    row_spec = P(("data", "expert"), None)
    weight_spec = P("expert", None, None)

    def device_step(token_rows, expert_ids, gate_weights, w_in, w_out):
        tokens, top_k = expert_ids.shape
        dim, hid = w_in.shape[1], w_in.shape[2]
        mean_load = tokens * top_k // groups
        slots = 7 * mean_load // 4
        cap = groups * mean_load
        any_spec = pl.BlockSpec(memory_space=pl.ANY)
        vmem_spec = pl.BlockSpec(memory_space=pltpu.VMEM)
        flops = 4 * groups * slots * dim * hid
        acc, tab, rfar = pl.pallas_call(
            functools.partial(layer_kernel, (groups, tokens, dim, hid, cap, slots)),
            out_shape=(
                jax.ShapeDtypeStruct((tokens, dim), F32),
                jax.ShapeDtypeStruct((tokens, 128), F32),
                jax.ShapeDtypeStruct((2, slots, dim), BF16),
                jax.ShapeDtypeStruct((groups, tokens, dim), BF16),
                jax.ShapeDtypeStruct((groups, slots, dim), BF16),
                jax.ShapeDtypeStruct((groups, slots, dim), BF16),
            ),
            in_specs=[any_spec, any_spec, vmem_spec, any_spec, any_spec],
            out_specs=(any_spec,) * 6,
            scratch_shapes=[
                pltpu.VMEM((groups, top_k, tokens), jnp.int32),
                pltpu.VMEM((groups, tokens), F32),
                pltpu.VMEM((tokens, 128), F32),
                pltpu.SemaphoreType.DMA((groups,)),
                pltpu.SemaphoreType.DMA((groups,)),
                pltpu.SemaphoreType.DMA((16,)),
                pltpu.SemaphoreType.DMA((2 * groups,)),
                pltpu.SemaphoreType.DMA((groups,)),
                pltpu.SemaphoreType.DMA((groups,)),
            ],
            compiler_params=pltpu.CompilerParams(collective_id=0, has_side_effects=True, vmem_limit_bytes=67043328),
            cost_estimate=pl.CostEstimate(flops=flops, bytes_accessed=400000000, transcendentals=0),
            name="layer",
        )(token_rows, expert_ids.T, gate_weights.T, w_in.reshape(dim, hid), w_out.reshape(hid, dim))[:3]
        rows = tokens // 4
        return pl.pallas_call(
            functools.partial(finish_kernel, 2 * groups),
            grid=(tokens // rows,),
            in_specs=[
                pl.BlockSpec((rows, dim), lambda i: (i, 0)),
                pl.BlockSpec((rows, 128), lambda i: (i, 0)),
                pl.BlockSpec((2, slots, dim), lambda i: (0, 0, 0)),
            ],
            out_specs=pl.BlockSpec((rows, dim), lambda i: (i, 0)),
            out_shape=jax.ShapeDtypeStruct((tokens, dim), BF16),
            cost_estimate=pl.CostEstimate(flops=4 * tokens * slots * dim, bytes_accessed=20000000, transcendentals=0),
            name="finish",
        )(acc, tab, rfar)

    return jax.shard_map(device_step, mesh=mesh, in_specs=(row_spec, row_spec, row_spec, weight_spec, weight_spec), out_specs=row_spec, check_vma=False)
```

```python
import functools

import jax
import jax.numpy as jnp
from jax import lax
from jax.experimental import pallas as pl
from jax.experimental.pallas import tpu as pltpu
from jax.sharding import PartitionSpec as P

MESH = pl.DeviceIdType.MESH
F32 = jnp.float32
BF16 = jnp.bfloat16


def layer_kernel(cfg, x_ref, ids_ref, gates_ref, win_ref, wout_ref, out_ref, ag_ref, obuf_ref, rbuf_ref,
                 ids_all, slot_tab, comb_tab, ids_send, ids_recv, ag_send, ag_recv, ret_send, ret_recv, barrier_unused=None):
    groups, tokens, dim, hid, cap, slots = cfg
    half = tokens // 2
    chips = groups // 2
    wchunk = 768
    nfull = hid // wchunk
    tail = hid - nfull * wchunk
    ochunks = dim // wchunk

    me = lax.axis_index("expert")
    chip = me // 2
    core = me % 2
    other = 1 - core
    sgn = 1 - 2 * core

    def dev(off, c):
        return ((chip + off + 2 * chips) % chips) * 2 + c

    sib = dev(0, other)
    src_a = dev(-sgn, core)
    src_b = dev(sgn, core)
    far = dev(2, core)

    def tile_dev(t, flip):
        q = t // 2
        p = t % 2
        f1 = q * (2 - q) * (3 - q) // 2
        f2 = q * (q - 1) * (3 - q) // 2
        f3 = q * (q - 1) * (q - 2) // 6
        off = flip * (f1 * (2 * p - 1) + f2 * (1 - 2 * p)) * sgn + 2 * f3
        c = core * (1 - p) + other * p
        return dev(off, c)

    def comb_dev(k):
        q = k // 2
        p = k % 2
        f1 = q * (2 - q) * (3 - q) // 2
        f2 = q * (q - 1) * (3 - q) // 2
        f3 = q * (q - 1) * (q - 2) // 6
        off = (f1 - f2) * sgn + 2 * f3
        c = core * (1 - p) + other * p
        return dev(off, c)

    def order(s):
        late = s // 5
        return s * (1 - late) + late * (5 + (s + 2) % 3)

    def remote(src, dst, ssem, rsem, target):
        return pltpu.make_async_remote_copy(src_ref=src, dst_ref=dst, send_sem=ssem, recv_sem=rsem,
                                            device_id={"expert": target}, device_id_type=MESH)

    bar = pltpu.get_barrier_semaphore()
    for k in range(1, groups):
        pl.semaphore_signal(bar, inc=1, device_id={"expert": (me + k) % groups}, device_id_type=MESH)
    pl.semaphore_wait(bar, groups - 1)

    def ids_copy(k):
        return remote(ids_ref, ids_all.at[me], ids_send.at[k - 1], ids_recv.at[me], (me + k) % groups)

    def ag_copy(src, d, h, k, target):
        return remote(src, ag_ref.at[d, pl.ds(h * half, half)], ag_send.at[k], ag_recv.at[2 * d + h], target)

    def own_half(h):
        return x_ref.at[pl.ds(h * half, half)]

    def got_half(d, h):
        return ag_ref.at[d, pl.ds(h * half, half)]

    half_a = (1 - sgn) // 2
    half_b = 1 - half_a
    send_sib = [ag_copy(own_half(h), me, h, h, sib) for h in range(2)]
    send_a = [ag_copy(own_half(h), me, h, 2 + h, src_b) for h in range(2)]
    send_b1 = ag_copy(own_half(half_b), me, half_b, 4, src_a)
    send_b2 = ag_copy(own_half(half_a), me, half_a, 5, src_a)
    fwd_a = ag_copy(got_half(src_a, half_a), src_a, half_a, 6, src_b)
    fwd_b = ag_copy(got_half(src_b, half_b), src_b, half_b, 7, src_a)
    pass_a = [ag_copy(got_half(src_a, h), src_a, h, 8 + h, sib) for h in range(2)]
    pass_b1 = ag_copy(got_half(src_b, half_b), src_b, half_b, 10, sib)
    pass_b2 = ag_copy(got_half(src_b, half_a), src_b, half_a, 11, sib)
    pass_f1 = ag_copy(got_half(far, half_a), far, half_a, 12, sib)
    pass_f2 = ag_copy(got_half(far, half_b), far, half_b, 13, sib)
    all_sends = send_sib + send_a + [send_b1, send_b2, fwd_a, fwd_b] + pass_a + [pass_b1, pass_b2, pass_f1, pass_f2]

    def wait_half(d, h):
        ag_copy(got_half(d, h), d, h, 0, sib).wait_recv()

    def ret_copy(t):
        d = tile_dev(t, 1)
        return remote(obuf_ref.at[d], rbuf_ref.at[me], ret_send.at[t], ret_recv.at[me], d)

    for k in range(1, groups):
        ids_copy(k).start()
    for c in send_sib + send_a:
        c.start()

    def compute(xsrc, xg, hbuf, pact, wbuf, wout, ostage, pbuf, xsem, wsem, osem, stsem, isem):
        own_ids = pltpu.make_async_copy(ids_ref, ids_all.at[me], isem)
        own_ids.start()

        def win_full(i):
            return pltpu.make_async_copy(win_ref.at[:, pl.ds(pl.multiple_of(i * wchunk, 128), wchunk)], wbuf.at[i % 2], wsem.at[i % 2])

        win_tail = pltpu.make_async_copy(win_ref.at[:, pl.ds(nfull * wchunk, tail)], wbuf.at[nfull % 2, :, pl.ds(0, tail)], wsem.at[nfull % 2])

        def wout_part(n):
            return pltpu.make_async_copy(wout_ref.at[:, pl.ds(pl.multiple_of(n * wchunk, 128), wchunk)], wout.at[:, pl.ds(pl.multiple_of(n * wchunk, 128), wchunk)], osem.at[n])

        win_full(0).start()
        for n in range(ochunks):
            wout_part(n).start()

        own_ids.wait()
        for k in range(1, groups):
            ids_copy(k).wait_send()
        for k in range(1, groups):
            d = (me + k) % groups
            remote(ids_ref, ids_all.at[d], ids_send.at[0], ids_recv.at[d], sib).wait_recv()
        ids0 = ids_all[:, 0, :]
        ids1 = ids_all[:, 1, :]
        o0 = ids_ref_v(ids_all, me, 0)
        o1 = ids_ref_v(ids_all, me, 1)
        eidx = lax.broadcasted_iota(jnp.int32, (groups, tokens), 0)

        def ind(m):
            return jnp.where(m, 1.0, 0.0).astype(F32)

        m0 = ind(ids0 == me)
        m1 = ind(ids1 == me)
        n0 = ind(o0 == eidx)
        n1 = ind(o1 == eidx)
        stack = jnp.concatenate([m0, m1, n0, n1], axis=0).astype(BF16)
        tri = ind(lax.broadcasted_iota(jnp.int32, (tokens, tokens), 0) < lax.broadcasted_iota(jnp.int32, (tokens, tokens), 1)).astype(BF16)
        pre = jnp.dot(stack, tri, preferred_element_type=F32)
        s0, s1, r0, r1 = [pre[k * groups:(k + 1) * groups] for k in range(4)]
        c0 = jnp.sum(m0, axis=1, keepdims=True)
        c1 = jnp.sum(m1, axis=1, keepdims=True)
        k0 = jnp.sum(n0, axis=1, keepdims=True)
        run0 = jnp.zeros((1, 1), F32)
        run1 = jnp.zeros((1, 1), F32)
        b0 = []
        b1 = []
        for d in range(groups):
            b0.append(run0)
            b1.append(run1)
            run0 = run0 + c0[d:d + 1]
            run1 = run1 + c1[d:d + 1]
        before0 = jnp.concatenate(b0, axis=0)
        before1 = jnp.concatenate(b1, axis=0) + run0
        keep0 = jnp.logical_and(m0 > 0, before0 + s0 < cap)
        keep1 = jnp.logical_and(m1 > 0, before1 + s1 < cap)
        slot_tab[...] = jnp.where(keep0, s0, jnp.where(keep1, c0 + s1, -1.0))

        dmask = ind(eidx < me)
        g0 = []
        g1 = []
        for e in range(groups):
            a0 = ind(ids0 == e)
            a1 = ind(ids1 == e)
            g0.append(jnp.sum(jnp.sum(a0 * dmask, axis=1, keepdims=True), axis=0, keepdims=True))
            g1.append(jnp.sum(jnp.sum(a0 + a1 * dmask, axis=1, keepdims=True), axis=0, keepdims=True))
        own0 = jnp.logical_and(n0 > 0, jnp.concatenate(g0, axis=0) + r0 < cap)
        own1 = jnp.logical_and(n1 > 0, jnp.concatenate(g1, axis=0) + r1 < cap)
        slot_own = jnp.where(own0, r0, jnp.where(own1, k0 + r1, -1.0))
        gate_own = n0 * gates_ref[0:1, :] + n1 * gates_ref[1:2, :]
        both = jnp.concatenate([slot_own, gate_own, jnp.zeros((128 - 2 * groups, tokens), F32)], axis=0)
        comb_tab[...] = jnp.transpose(both)

        def stage_copy_own():
            return pltpu.make_async_copy(ostage, rbuf_ref.at[me], stsem)

        def stage_copy(t):
            return pltpu.make_async_copy(ostage, obuf_ref.at[tile_dev(t, 1)], stsem)

        def tile(s, carry):
            t = order(s)
            d = tile_dev(t, 1)

            @pl.when(t % 2 == 1)
            def _():
                wait_half(d, 0)
                wait_half(d, 1)

            def xcols(n):
                return pl.ds(pl.multiple_of(n * wchunk, 128), wchunk)

            def x_start(n):
                @pl.when(s == 0)
                def _():
                    pltpu.make_async_copy(x_ref.at[:, xcols(n)], xsrc.at[n % 2], xsem.at[n % 2]).start()

                @pl.when(s > 0)
                def _():
                    pltpu.make_async_copy(ag_ref.at[d, :, xcols(n)], xsrc.at[n % 2], xsem.at[n % 2]).start()

            x_start(0)
            row = slot_tab[pl.ds(d, 1), :]
            pbuf[...] = jnp.where(lax.broadcasted_iota(jnp.int32, (slots, tokens), 0).astype(F32) == row, 1.0, 0.0).astype(BF16)

            def gather(n, cc):
                @pl.when(n + 1 < ochunks)
                def _():
                    x_start(n + 1)
                pltpu.make_async_copy(x_ref.at[:, xcols(n)], xsrc.at[n % 2], xsem.at[n % 2]).wait()
                xg[:, xcols(n)] = jnp.dot(pbuf[...], xsrc[n % 2], preferred_element_type=F32).astype(BF16)
                return cc

            lax.fori_loop(0, ochunks, gather, 0)

            def up(i, cc):
                @pl.when(jnp.logical_and(s == 1, i == 2))
                def _():
                    stage_copy_own().wait()
                    wait_half(src_a, 0)
                    pass_a[0].start()

                @pl.when(jnp.logical_and(s == 3, i == 3))
                def _():
                    wait_half(src_b, half_b)
                    fwd_b.start()
                    pass_b1.start()

                @pl.when(jnp.logical_and(s == 4, i == 3))
                def _():
                    wait_half(far, half_a)
                    pass_f1.start()

                @pl.when(jnp.logical_and(s > 1, i == 1))
                def _():
                    stage_copy(order(s - 1)).wait()

                    @pl.when(s != 3)
                    def _():
                        ret_copy(order(s - 1)).start()

                @pl.when(i + 1 < nfull)
                def _():
                    win_full(i + 1).start()

                @pl.when(i + 1 == nfull)
                def _():
                    win_tail.start()

                win_full(i).wait()
                prev = pl.ds(pl.multiple_of((i - 1) * wchunk, 128), wchunk)
                hbuf[:, prev] = jax.nn.gelu(pact[(i - 1) % 2]).astype(BF16)
                pact[i % 2] = jnp.dot(xg[...], wbuf[i % 2], preferred_element_type=F32)
                return cc

            win_full(1).start()
            win_full(0).wait()
            pact[0] = jnp.dot(xg[...], wbuf[0], preferred_element_type=F32)
            lax.fori_loop(1, nfull, up, 0)
            win_tail.wait()

            @pl.when(s + 1 < groups)
            def _():
                win_full(0).start()
            hbuf[:, (nfull - 1) * wchunk:nfull * wchunk] = jax.nn.gelu(pact[(nfull - 1) % 2]).astype(BF16)
            pre_act = jnp.dot(xg[...], wbuf[nfull % 2, :, 0:tail], preferred_element_type=F32)
            hbuf[:, nfull * wchunk:hid] = jax.nn.gelu(pre_act).astype(BF16)

            def down(n, cc):
                @pl.when(s == 0)
                def _():
                    wout_part(n).wait()

                @pl.when(jnp.logical_and(s == 1, n == 0))
                def _():
                    send_b1.start()
                    send_b2.start()
                    wait_half(src_a, 1)
                    fwd_a.start()
                    pass_a[1].start()

                @pl.when(jnp.logical_and(s == 3, n == 2))
                def _():
                    wait_half(src_b, half_a)
                    pass_b2.start()
                    ret_copy(2).start()

                @pl.when(jnp.logical_and(s == 4, n == 0))
                def _():
                    wait_half(far, half_b)
                    pass_f2.start()

                cols = pl.ds(pl.multiple_of(n * wchunk, 128), wchunk)
                ostage[:, cols] = jnp.dot(hbuf[...], wout[:, cols], preferred_element_type=F32).astype(BF16)
                return cc

            lax.fori_loop(0, ochunks, down, 0)

            @pl.when(s == 0)
            def _():
                stage_copy_own().start()

            @pl.when(s > 0)
            def _():
                stage_copy(t).start()
            return carry

        lax.fori_loop(0, groups, tile, 0)
        stage_copy(order(groups - 1)).wait()
        ret_copy(order(groups - 1)).start()

    def ids_ref_v(ref, d, j):
        return ref[pl.ds(d, 1), j, :]

    pl.run_scoped(
        compute,
        pltpu.VMEM((2, tokens, wchunk), BF16),
        pltpu.VMEM((slots, dim), BF16),
        pltpu.VMEM((slots, hid), BF16),
        pltpu.VMEM((2, slots, wchunk), F32),
        pltpu.VMEM((2, dim, wchunk), BF16),
        pltpu.VMEM((hid, dim), BF16),
        pltpu.VMEM((slots, dim), BF16),
        pltpu.VMEM((slots, tokens), BF16),
        pltpu.SemaphoreType.DMA((2,)),
        pltpu.SemaphoreType.DMA((2,)),
        pltpu.SemaphoreType.DMA((ochunks,)),
        pltpu.SemaphoreType.DMA(()),
        pltpu.SemaphoreType.DMA(()),
    )

    def combine(acc, xb, rb, qbuf, xsem, rsem, osem):
        x_in = pltpu.make_async_copy(x_ref, xb, xsem)
        x_in.start()
        x_in.wait()
        for n in range(ochunks):
            cols = slice(n * wchunk, (n + 1) * wchunk)
            acc[:, cols] = xb[:, cols].astype(F32)

        def block_copy(k):
            return pltpu.make_async_copy(rbuf_ref.at[comb_dev(order(k))], rb.at[k % 2], rsem.at[k % 2])

        def block_ready(k):
            e = comb_dev(order(k))
            remote(obuf_ref.at[e], rbuf_ref.at[e], ret_send.at[0], ret_recv.at[e], sib).wait_recv()
            block_copy(k).start()

        block_copy(0).start()

        def add_block(k, cc):
            e = comb_dev(order(k))

            @pl.when(k < groups - 2)
            def _():
                block_ready(k + 1)
            lane = lax.broadcasted_iota(jnp.int32, (tokens, 128), 1)
            tab = comb_tab[...]
            slot_col = jnp.sum(jnp.where(lane == e, tab, 0.0), axis=1, keepdims=True)
            gate_col = jnp.sum(jnp.where(lane == e + groups, tab, 0.0), axis=1, keepdims=True)
            qbuf[...] = jnp.where(lax.broadcasted_iota(jnp.int32, (tokens, slots), 1).astype(F32) == slot_col, 1.0, 0.0).astype(BF16)
            block_copy(k).wait()

            def part(n, c2):
                cols = pl.ds(pl.multiple_of(n * wchunk, 128), wchunk)
                pick = jnp.dot(qbuf[...], rb[k % 2, :, cols], preferred_element_type=F32)
                acc[:, cols] = acc[:, cols] + gate_col * pick
                return c2

            lax.fori_loop(0, ochunks, part, 0)

            @pl.when(k == groups - 2)
            def _():
                block_ready(k + 1)
            return cc

        lax.fori_loop(0, groups, add_block, 0)
        xb[...] = acc[...].astype(BF16)
        fin = pltpu.make_async_copy(xb, out_ref, osem)
        fin.start()
        fin.wait()

    pl.run_scoped(
        combine,
        pltpu.VMEM((tokens, dim), F32),
        pltpu.VMEM((tokens, dim), BF16),
        pltpu.VMEM((2, slots, dim), BF16),
        pltpu.VMEM((tokens, slots), BF16),
        pltpu.SemaphoreType.DMA(()),
        pltpu.SemaphoreType.DMA((2,)),
        pltpu.SemaphoreType.DMA(()),
    )

    for c in all_sends:
        c.wait_send()
    for t in range(1, groups):
        ret_copy(t).wait_send()


def solution(mesh):
    groups = mesh.shape["expert"]
    row_spec = P(("data", "expert"), None)
    weight_spec = P("expert", None, None)

    def device_step(token_rows, expert_ids, gate_weights, w_in, w_out):
        tokens, top_k = expert_ids.shape
        dim, hid = w_in.shape[1], w_in.shape[2]
        mean_load = tokens * top_k // groups
        slots = 7 * mean_load // 4
        cap = groups * mean_load
        any_spec = pl.BlockSpec(memory_space=pl.ANY)
        vmem_spec = pl.BlockSpec(memory_space=pltpu.VMEM)
        flops = 4 * groups * slots * dim * hid
        out = pl.pallas_call(
            functools.partial(layer_kernel, (groups, tokens, dim, hid, cap, slots)),
            out_shape=(
                jax.ShapeDtypeStruct((tokens, dim), BF16),
                jax.ShapeDtypeStruct((groups, tokens, dim), BF16),
                jax.ShapeDtypeStruct((groups, slots, dim), BF16),
                jax.ShapeDtypeStruct((groups, slots, dim), BF16),
            ),
            in_specs=[any_spec, any_spec, vmem_spec, any_spec, any_spec],
            out_specs=(any_spec, any_spec, any_spec, any_spec),
            scratch_shapes=[
                pltpu.VMEM((groups, top_k, tokens), jnp.int32),
                pltpu.VMEM((groups, tokens), F32),
                pltpu.VMEM((tokens, 128), F32),
                pltpu.SemaphoreType.DMA((groups,)),
                pltpu.SemaphoreType.DMA((groups,)),
                pltpu.SemaphoreType.DMA((16,)),
                pltpu.SemaphoreType.DMA((2 * groups,)),
                pltpu.SemaphoreType.DMA((groups,)),
                pltpu.SemaphoreType.DMA((groups,)),
            ],
            compiler_params=pltpu.CompilerParams(collective_id=0, has_side_effects=True, vmem_limit_bytes=67043328),
            cost_estimate=pl.CostEstimate(flops=flops, bytes_accessed=400000000, transcendentals=0),
            name="layer",
        )(token_rows, expert_ids.T, gate_weights.T, w_in.reshape(dim, hid), w_out.reshape(hid, dim))
        return out[0]

    return jax.shard_map(device_step, mesh=mesh, in_specs=(row_spec, row_spec, row_spec, weight_spec, weight_spec), out_specs=row_spec, check_vma=False)
```
